32 devices in a mesh: depth: 8 (over z, x), rows: 4 (over y, core).
Axes of the slice: x: 2, y: 2, z: 4, core: 2. Of those that a mesh axis runs over, the one named last changes fastest.
Arguments:
- density: float32 [128, 64, 1024], P('depth', 'rows'), may hold values from 0 to 1
- bin_of_level: int32 [16], replicated, may hold values from 0 to 7
- absorb_bins: float32 [8], replicated, may hold values from 0.00234375 to 0.0625
- emit_bins: float32 [8], replicated, may hold values from 0.2 to 3
- occupancy: int32 [8, 4, 8], P('depth', 'rows'), may hold values 0 or 1
- col_offsets: int32 [1024], replicated, may hold values from 2 to 6
- row_offsets: int32 [64], P('rows'), may hold values from 2 to 6
Outputs:
- front_transmittance: float32 [8, 64, 1024], P('depth', 'rows')
- final_image: float32 [2, 64, 1024], P(None, 'rows')
The draws below stay inside these ranges and needn't reach their ends.
All inputs are finite; a program needn't handle non-finite values. No bound on the sum of `occupancy` on one device may be relied on, other than what follows from the above.
Results may differ from the reference program's by a relative error of at most 0.0002.
Values sent between devices are 32-bit elements; how exact they have to be, the bound alone decides.
A program may use at most 64 MiB of HBM per device.

```python
import math
import jax
import jax.numpy as jnp
from jax import lax

COLS = 1024
LEVELS = 16
BINS = 8
SLAB = 16
ROW_DEV = 16
DEPTH_ALL = 128
ROWS_ALL = 64
TILES = 8
N_DEPTH = 8
N_ROWS = 4


def set_ends(entries, rng, smallest, top_value):
    place = [jax.random.randint(jax.random.fold_in(rng, axis), (), 0, length) for axis, length in enumerate(entries.shape)]
    widest = entries.shape.index(max(entries.shape))
    beside = place[:widest] + [(place[widest] + 1) % entries.shape[widest]] + place[widest + 1:]
    return entries.at[tuple(place)].set(smallest).at[tuple(beside)].set(top_value)


def block_scale(rng, shape, shards, least, largest):
    gain, own = 1.0, jax.random.fold_in(rng, 6)
    for axis_at, blocks in shards:
        heights = jnp.exp(jax.random.uniform(jax.random.fold_in(own, axis_at), (blocks,), jnp.float32, least / len(shards), largest / len(shards)))
        gain = gain * jnp.repeat(heights, shape[axis_at] // blocks).reshape([-1 if axis == axis_at else 1 for axis in range(len(shape))])
    return gain


def setup_inputs(seed: int = 0) -> dict:
    key_list = jax.random.split(jax.random.key(seed), 8)
    return {
        "density": jnp.clip(1.0 * jax.random.uniform(key_list[0], (DEPTH_ALL, ROWS_ALL, COLS), jnp.float32) ** block_scale(key_list[0], (DEPTH_ALL, ROWS_ALL, COLS), ((0, 8), (1, 4)), -0.2, 0.2), 0.0, 1.0),
        "bin_of_level": set_ends(jax.random.randint(key_list[1], (LEVELS,), 0, BINS), jax.random.fold_in(key_list[1], 1), 0, BINS - 1).astype(jnp.int32),
        "absorb_bins": jnp.clip(jnp.exp(jax.random.uniform(key_list[2], (BINS,), jnp.float32, math.log(0.00234375), math.log(0.0625))), 0.00234375, 0.0625),
        "emit_bins": jnp.clip(jnp.exp(jax.random.uniform(key_list[3], (BINS,), jnp.float32, math.log(0.2), math.log(3.0))), 0.2, 3.0),
        "occupancy": set_ends((jax.random.randint(key_list[4], (N_DEPTH, N_ROWS, TILES), 0, 4) < 3).astype(jnp.int32), jax.random.fold_in(key_list[4], 1), 0, 1),
        "col_offsets": set_ends(jax.random.randint(key_list[5], (COLS,), 2, 7), jax.random.fold_in(key_list[5], 1), 2, 6).astype(jnp.int32),
        "row_offsets": set_ends(jax.random.randint(key_list[6], (ROWS_ALL,), 2, 7), jax.random.fold_in(key_list[6], 1), 2, 6).astype(jnp.int32),
    }


def resample_columns(mixed, col_offsets):
    fraction = col_offsets.astype(jnp.float32) / 8.0
    pad_shape = mixed.shape[:-1] + (1,)
    right_side = jnp.concatenate([mixed[..., 1:], jnp.zeros(pad_shape, jnp.float32)], -1)
    return (1.0 - fraction) * mixed + fraction * right_side


def tables(bin_of_level, absorb_bins, emit_bins):
    count_bins = absorb_bins.shape[0]
    onehot = (bin_of_level[:, None] == jnp.arange(count_bins, dtype=jnp.int32)[None, :]).astype(jnp.float32)
    return jnp.sum(onehot * absorb_bins[None, :], 1), jnp.sum(onehot * emit_bins[None, :], 1)


def classify(sampled, absorb_level, emit_level):
    levels = absorb_level.shape[0]
    scaled = sampled * float(levels - 1)
    absorption = jnp.zeros(sampled.shape, jnp.float32)
    emission = jnp.zeros(sampled.shape, jnp.float32)
    for knot_index in range(levels):
        weight = jnp.maximum(0.0, 1.0 - jnp.abs(scaled - float(knot_index)))
        absorption = absorption + weight * absorb_level[knot_index]
        emission = emission + weight * emit_level[knot_index]
    return absorption, emission


def composite(absorption, emission):
    inclusive = jnp.cumsum(absorption, 0)
    exclusive = inclusive - absorption
    light = jnp.sum(jnp.exp(-exclusive) * (1.0 - jnp.exp(-absorption)) * emission, 0)
    return light, inclusive[-1]


def reference(density, bin_of_level, absorb_bins, emit_bins, occupancy, col_offsets, row_offsets):
    absorb_level, emit_level = tables(bin_of_level, absorb_bins, emit_bins)
    frac_row = (row_offsets.astype(jnp.float32) / 8.0)[None, :, None]
    slabs = density.reshape(N_DEPTH, SLAB, ROWS_ALL, COLS)
    followers = jnp.concatenate([slabs[1:, 0], jnp.zeros((1, ROWS_ALL, COLS), jnp.float32)], 0)

    def per_slab(inputs):
        planes, following, occupied = inputs
        extended = jnp.concatenate([planes, following[None]], 0)
        mid_depth = 0.5 * (extended[:-1] + extended[1:])
        next_rows = jnp.concatenate([mid_depth[:, 1:], jnp.zeros((SLAB, 1, COLS), jnp.float32)], 1)
        mixed = (1.0 - frac_row) * mid_depth + frac_row * next_rows
        sampled = resample_columns(mixed, col_offsets)
        absorption, emission = classify(sampled, absorb_level, emit_level)
        brick_mask = jnp.repeat(jnp.repeat(occupied.astype(jnp.float32), ROW_DEV, 0), 128, 1)
        absorption = absorption * brick_mask[None]
        return composite(absorption, emission)

    lights, depths = lax.map(per_slab, (slabs, followers, occupancy))
    front_depth = jnp.cumsum(depths, 0) - depths
    front = jnp.exp(-front_depth)
    radiance = jnp.sum(front * lights, 0)
    remaining = jnp.exp(-jnp.sum(depths, 0))
    return front, jnp.stack([radiance, remaining])
```

```python
import functools
import math

import jax
import jax.numpy as jnp
from jax import lax
from jax.experimental import pallas as pl
from jax.experimental.pallas import tpu as pltpu
from jax.sharding import PartitionSpec as P

LANES = 128
SUB = 8
MESH = pl.DeviceIdType.MESH


def repeat(count, body):
    if count <= 16:
        for i in range(count):
            body(i)
    else:
        lax.fori_loop(0, count, lambda i, c: (body(i), c)[1], 0)


def kernel(
    n_depth,
    n_rows,
    dens_hbm,
    bins_ref,
    absorb_ref,
    emit_ref,
    occ_ref,
    col_ref,
    row_ref,
    front_ref,
    image_ref,
    dens,
    below,
    row_send,
    row_halo,
    corner_send,
    corner,
    parts,
    gathered,
    answers,
    results,
    load_sem,
    halo_send_sem,
    halo_recv_sem,
    part_send_sem,
    part_recv_sem,
    ans_send_sem,
    ans_recv_sem,
):
    slab, rows, cols = dens.shape
    owners = parts.shape[0]
    width = cols // owners
    tiles = cols // LANES
    row_tiles = rows // SUB
    levels = bins_ref.shape[0]
    d = lax.axis_index("depth")
    r = lax.axis_index("rows")

    def shifted(dd, dr):
        return (lax.rem(d + dd + n_depth, n_depth), lax.rem(r + dr + n_rows, n_rows))

    load = pltpu.make_async_copy(dens_hbm, dens, load_sem)
    load.start()

    barrier = pltpu.get_barrier_semaphore()
    for dd, dr in ((0, -1), (0, 1), (-1, -1), (1, 1)):
        pl.semaphore_signal(barrier, inc=1, device_id=shifted(dd, dr), device_id_type=MESH)

    def greet(i):
        pl.semaphore_signal(
            barrier, inc=1, device_id=(lax.rem(d + 1 + i, n_depth), r), device_id_type=MESH
        )

    repeat(n_depth - 1, greet)

    @pl.when(d == n_depth - 1)
    def _():
        below[...] = jnp.zeros_like(below)

    @pl.when(r == n_rows - 1)
    def _():
        row_halo[...] = jnp.zeros_like(row_halo)

    @pl.when(jnp.logical_or(d == n_depth - 1, r == n_rows - 1))
    def _():
        corner[...] = jnp.zeros_like(corner)

    lane = lax.broadcasted_iota(jnp.int32, (SUB, LANES), 1)
    sub = lax.broadcasted_iota(jnp.int32, (SUB, LANES), 0)
    to_log2 = -math.log2(math.e)
    absorb = [absorb_ref[bins_ref[k]] * to_log2 for k in range(levels)]
    emit = [emit_ref[bins_ref[k]] for k in range(levels)]

    def table(values):
        base = jnp.full((SUB, LANES), values[-1], jnp.float32)
        slope = jnp.zeros((SUB, LANES), jnp.float32)
        for k in range(levels - 1):
            step = values[k + 1] - values[k]
            base = jnp.where(lane == k, values[k] - step * float(k), base)
            slope = jnp.where(lane == k, step, slope)
        return base, slope

    a_base, a_slope = table(absorb)
    e_base, e_slope = table(emit)
    occ = [occ_ref[0, 0, (c * LANES) // (cols // occ_ref.shape[2])].astype(jnp.float32) for c in range(tiles)]

    def row_weights(t):
        frac = jnp.zeros((SUB, LANES), jnp.float32)
        for y in range(SUB):
            frac = jnp.where(sub == y, row_ref[t * SUB + y].astype(jnp.float32), frac)
        frac = frac / 8.0
        gain = 0.5 * float(levels - 1)
        return gain * (1.0 - frac), gain * frac

    def col_weights(c):
        frac = col_ref[0:1, c * LANES : (c + 1) * LANES].astype(jnp.float32) / 8.0
        frac = jnp.broadcast_to(frac, (SUB, LANES))
        keep = 1.0 - frac
        if c == tiles - 1:
            frac = jnp.where(lane == LANES - 1, 0.0, frac)
        return keep, frac

    def resampled(own, following, rw, cws):
        mixed = []
        for c in range(tiles):
            block = own(c)
            up = jnp.where(sub == SUB - 1, following(c), pltpu.roll(block, SUB - 1, 0))
            mixed.append(rw[0] * block + rw[1] * up)
        turned = [pltpu.roll(m, LANES - 1, 1) for m in mixed]
        out = []
        for c in range(tiles):
            right = jnp.where(lane == LANES - 1, turned[(c + 1) % tiles], turned[c])
            out.append(cws[c][0] * mixed[c] + cws[c][1] * right)
        return out

    def shade(prev, now, state):
        through, depth, light = state
        new_through, new_depth, new_light = [], [], []
        for c in range(tiles):
            scaled = prev[c] + now[c]
            level = scaled.astype(jnp.int32)
            pick = functools.partial(jnp.take_along_axis, indices=level, axis=1, mode="promise_in_bounds")
            absorbed = (pick(a_base) + pick(a_slope) * scaled) * occ[c]
            emitted = pick(e_base) + pick(e_slope) * scaled
            after = through[c] * jnp.exp2(absorbed)
            new_light.append(light[c] + (through[c] - after) * emitted)
            new_depth.append(depth[c] + absorbed)
            new_through.append(after)
        return new_through, new_depth, new_light

    cws = [col_weights(c) for c in range(tiles)]

    def tile_of(c):
        return slice(c * LANES, (c + 1) * LANES)

    def plane(z, t, rw):
        def own(c):
            return dens[z, t * SUB : (t + 1) * SUB, tile_of(c)]

        def following(c):
            if t + 1 < row_tiles:
                nxt = dens[z, (t + 1) * SUB : (t + 1) * SUB + 1, tile_of(c)]
            else:
                nxt = row_halo[z, 0:1, tile_of(c)]
            return jnp.broadcast_to(nxt, (SUB, LANES))

        return resampled(own, following, rw, cws)

    def last_plane(t, rw):
        def own(c):
            return below[t * SUB : (t + 1) * SUB, tile_of(c)]

        def following(c):
            if t + 1 < row_tiles:
                nxt = below[(t + 1) * SUB : (t + 1) * SUB + 1, tile_of(c)]
            else:
                nxt = corner[0:1, tile_of(c)]
            return jnp.broadcast_to(nxt, (SUB, LANES))

        return resampled(own, following, rw, cws)

    def march(t):
        rw = row_weights(t)
        ones = [jnp.ones((SUB, LANES), jnp.float32)] * tiles
        zeros = [jnp.zeros((SUB, LANES), jnp.float32)] * tiles

        def step(z, carry):
            prev, state = carry
            now = plane(z, t, rw)
            return now, shade(prev, now, state)

        return lax.fori_loop(1, slab, step, (plane(0, t, rw), (ones, zeros, zeros)))

    def finish(t, carry):
        prev, state = carry
        _, depth, light = shade(prev, last_plane(t, row_weights(t)), state)
        for c in range(tiles):
            j, at = (c * LANES) // width, (c * LANES) % width
            parts[j, 0, t * SUB : (t + 1) * SUB, at : at + LANES] = depth[c]
            parts[j, 1, t * SUB : (t + 1) * SUB, at : at + LANES] = light[c]

    load.wait()
    for z in range(slab):
        row_send[z] = dens[z, 0:1, :]
    corner_send[...] = dens[0, 0:1, :]

    pl.semaphore_wait(barrier, n_depth - 1 + 4)

    def halo(k, src, dst, dd, dr):
        return pltpu.make_async_remote_copy(
            src_ref=src,
            dst_ref=dst,
            send_sem=halo_send_sem.at[k],
            recv_sem=halo_recv_sem.at[k],
            device_id=shifted(dd, dr),
            device_id_type=MESH,
        )

    depth_copy = halo(0, dens.at[0], below, -1, 0)
    rows_copy = halo(1, row_send, row_halo, 0, -1)
    corner_copy = halo(2, corner_send, corner, -1, -1)
    sends = (
        (depth_copy, d > 0, d < n_depth - 1),
        (rows_copy, r > 0, r < n_rows - 1),
        (
            corner_copy,
            jnp.logical_and(d > 0, r > 0),
            jnp.logical_and(d < n_depth - 1, r < n_rows - 1),
        ),
    )
    for copy, sending, _ in sends:
        pl.when(sending)(copy.start)

    halves = [march(t) for t in range(row_tiles - 1)]
    pl.when(sends[1][2])(rows_copy.wait_recv)
    halves.append(march(row_tiles - 1))
    pl.when(sends[0][2])(depth_copy.wait_recv)
    pl.when(sends[2][2])(corner_copy.wait_recv)
    for t, carry in enumerate(halves):
        finish(t, carry)

    def part_copy(owner, source):
        return pltpu.make_async_remote_copy(
            src_ref=parts.at[owner],
            dst_ref=gathered.at[source],
            send_sem=part_send_sem.at[owner],
            recv_sem=part_recv_sem.at[source],
            device_id=(owner, r),
            device_id_type=MESH,
        )

    def other(i):
        return lax.rem(d + 1 + i, n_depth)

    def when_owner(index, body):
        if owners == n_depth:
            body()
        else:
            pl.when(index < owners)(body)

    def send_part(i):
        when_owner(other(i), lambda: part_copy(other(i), d).start())

    repeat(n_depth - 1, send_part)

    def answer_copy(target, owner):
        return pltpu.make_async_remote_copy(
            src_ref=answers.at[target],
            dst_ref=results.at[owner],
            send_sem=ans_send_sem.at[target],
            recv_sem=ans_recv_sem.at[owner],
            device_id=(target, r),
            device_id_type=MESH,
        )

    @functools.partial(when_owner, d)
    def _():
        gathered[pl.ds(d, 1)] = parts[pl.ds(d, 1)]

        def arrived(i):
            part_copy(d, other(i)).wait_recv()

        repeat(n_depth - 1, arrived)

        def compose(i, carry):
            total, radiance = carry
            front = jnp.exp2(total)
            answers[i, 0] = front
            return total + gathered[i, 0], radiance + front * gathered[i, 1]

        zero = jnp.zeros((rows, width), jnp.float32)
        carry = (zero, zero)
        if n_depth <= 16:
            for i in range(n_depth):
                carry = compose(i, carry)
        else:
            carry = lax.fori_loop(0, n_depth, compose, carry)
        total, radiance = carry
        remaining = jnp.exp2(total)

        def fill(i):
            answers[i, 1] = radiance
            answers[i, 2] = remaining

        repeat(n_depth, fill)

        def reply(i):
            answer_copy(other(i), d).start()

        repeat(n_depth - 1, reply)
        results[pl.ds(d, 1)] = answers[pl.ds(d, 1)]

    def collect(i):
        when_owner(other(i), lambda: answer_copy(d, other(i)).wait_recv())

    repeat(n_depth - 1, collect)
    for j in range(owners):
        where = slice(j * width, (j + 1) * width)
        front_ref[0, :, where] = results[j, 0]
        image_ref[0, :, where] = results[j, 1]
        image_ref[1, :, where] = results[j, 2]

    for copy, sending, _ in sends:
        pl.when(sending)(copy.wait_send)

    def sent(i):
        when_owner(other(i), lambda: part_copy(other(i), d).wait_send())
        when_owner(d, lambda: answer_copy(other(i), d).wait_send())

    repeat(n_depth - 1, sent)


def on_device(n_depth, n_rows, density, bin_of_level, absorb_bins, emit_bins, occupancy, col_offsets, row_offsets):
    slab, rows, cols = density.shape
    owners = 1
    while owners * 2 <= n_depth and cols % (owners * 2 * LANES) == 0:
        owners *= 2
    width = cols // owners
    smem = pl.BlockSpec(memory_space=pltpu.SMEM)
    vmem = pl.BlockSpec(memory_space=pltpu.VMEM)
    f32 = jnp.float32
    return pl.pallas_call(
        functools.partial(kernel, n_depth, n_rows),
        out_shape=(
            jax.ShapeDtypeStruct((1, rows, cols), f32),
            jax.ShapeDtypeStruct((2, rows, cols), f32),
        ),
        in_specs=[pl.BlockSpec(memory_space=pl.ANY), smem, smem, smem, smem, vmem, smem],
        out_specs=(vmem, vmem),
        scratch_shapes=[
            pltpu.VMEM((slab, rows, cols), f32),
            pltpu.VMEM((rows, cols), f32),
            pltpu.VMEM((slab, 1, cols), f32),
            pltpu.VMEM((slab, 1, cols), f32),
            pltpu.VMEM((1, cols), f32),
            pltpu.VMEM((1, cols), f32),
            pltpu.VMEM((owners, 2, rows, width), f32),
            pltpu.VMEM((n_depth, 2, rows, width), f32),
            pltpu.VMEM((n_depth, 3, rows, width), f32),
            pltpu.VMEM((owners, 3, rows, width), f32),
            pltpu.SemaphoreType.DMA,
            pltpu.SemaphoreType.DMA((3,)),
            pltpu.SemaphoreType.DMA((3,)),
            pltpu.SemaphoreType.DMA((owners,)),
            pltpu.SemaphoreType.DMA((n_depth,)),
            pltpu.SemaphoreType.DMA((n_depth,)),
            pltpu.SemaphoreType.DMA((owners,)),
        ],
        compiler_params=pltpu.CompilerParams(collective_id=0, has_side_effects=True),
    )(
        density,
        bin_of_level,
        absorb_bins,
        emit_bins,
        occupancy,
        col_offsets.reshape(1, cols),
        row_offsets,
    )


def solution(mesh):
    placed = (P("depth", "rows", None), P(), P(), P(), P("depth", "rows", None), P(), P("rows"))
    return jax.shard_map(
        functools.partial(on_device, mesh.shape["depth"], mesh.shape["rows"]),
        mesh=mesh,
        in_specs=placed,
        out_specs=(P("depth", "rows", None), P(None, "rows", None)),
        check_vma=False,
    )
```

```python
import functools
import math

import jax
import jax.numpy as jnp
from jax import lax
from jax.experimental import pallas as pl
from jax.experimental.pallas import tpu as pltpu
from jax.sharding import PartitionSpec as P

LANES = 128
SUB = 8
MESH = pl.DeviceIdType.MESH


def repeat(count, body):
    if count <= 16:
        for i in range(count):
            body(i)
    else:
        lax.fori_loop(0, count, lambda i, c: (body(i), c)[1], 0)


def kernel(
    n_depth,
    n_rows,
    dens_hbm,
    bins_ref,
    absorb_ref,
    emit_ref,
    occ_ref,
    col_ref,
    row_ref,
    results,
    dens,
    below,
    row_send,
    row_halo,
    corner_send,
    corner,
    parts,
    gathered,
    answers,
    load_sem,
    halo_send_sem,
    halo_recv_sem,
    part_send_sem,
    part_recv_sem,
    ans_send_sem,
    ans_recv_sem,
):
    slab, rows, cols = dens.shape
    owners = parts.shape[1]
    width = cols // owners
    tiles = cols // LANES
    row_tiles = rows // SUB
    levels = bins_ref.shape[0]
    d = lax.axis_index("depth")
    r = lax.axis_index("rows")

    def shifted(dd, dr):
        return (lax.rem(d + dd + n_depth, n_depth), lax.rem(r + dr + n_rows, n_rows))

    load = pltpu.make_async_copy(dens_hbm, dens, load_sem)
    load.start()

    barrier = pltpu.get_barrier_semaphore()
    for dd, dr in ((0, -1), (0, 1), (-1, -1), (1, 1)):
        pl.semaphore_signal(barrier, inc=1, device_id=shifted(dd, dr), device_id_type=MESH)

    def greet(i):
        pl.semaphore_signal(
            barrier, inc=1, device_id=(lax.rem(d + 1 + i, n_depth), r), device_id_type=MESH
        )

    repeat(n_depth - 1, greet)

    @pl.when(d == n_depth - 1)
    def _():
        below[...] = jnp.zeros_like(below)

    @pl.when(r == n_rows - 1)
    def _():
        row_halo[...] = jnp.zeros_like(row_halo)

    @pl.when(jnp.logical_or(d == n_depth - 1, r == n_rows - 1))
    def _():
        corner[...] = jnp.zeros_like(corner)

    lane = lax.broadcasted_iota(jnp.int32, (SUB, LANES), 1)
    sub = lax.broadcasted_iota(jnp.int32, (SUB, LANES), 0)
    to_log2 = -math.log2(math.e)
    absorb = [absorb_ref[bins_ref[k]] * to_log2 for k in range(levels)]
    emit = [emit_ref[bins_ref[k]] for k in range(levels)]

    def hinges(values):
        steps = [values[k + 1] - values[k] for k in range(levels - 1)]
        bend = steps[:1] + [steps[k] - steps[k - 1] for k in range(1, levels - 1)]
        shift = values[0]
        for k in range(1, levels - 1):
            shift = shift - bend[k] * float(k)
        return shift, bend

    a_shift, a_bend = hinges(absorb)
    e_shift, e_bend = hinges(emit)
    occ = [occ_ref[0, 0, (c * LANES) // (cols // occ_ref.shape[2])].astype(jnp.float32) for c in range(tiles)]

    def row_weights(t):
        frac = jnp.zeros((SUB, LANES), jnp.float32)
        for y in range(SUB):
            frac = jnp.where(sub == y, row_ref[t * SUB + y].astype(jnp.float32), frac)
        frac = frac / 8.0
        gain = 0.5 * float(levels - 1)
        return gain * (1.0 - frac), gain * frac

    def col_weights(c):
        frac = col_ref[0:1, c * LANES : (c + 1) * LANES].astype(jnp.float32) / 8.0
        frac = jnp.broadcast_to(frac, (SUB, LANES))
        keep = 1.0 - frac
        if c == tiles - 1:
            frac = jnp.where(lane == LANES - 1, 0.0, frac)
        return keep, frac

    def resampled(own, following, rw, cws):
        mixed = []
        for c in range(tiles):
            block = own(c)
            up = jnp.where(sub == SUB - 1, following(c), pltpu.roll(block, SUB - 1, 0))
            mixed.append(rw[0] * block + rw[1] * up)
        turned = [pltpu.roll(m, LANES - 1, 1) for m in mixed]
        out = []
        for c in range(tiles):
            right = jnp.where(lane == LANES - 1, turned[(c + 1) % tiles], turned[c])
            out.append(cws[c][0] * mixed[c] + cws[c][1] * right)
        return out

    def shade(prev, now, state):
        through, depth, light = state
        new_through, new_depth, new_light = [], [], []
        for c in range(tiles):
            scaled = prev[c] + now[c]
            absorbed = a_shift + a_bend[0] * scaled
            emitted = e_shift + e_bend[0] * scaled
            for k in range(1, levels - 1):
                hinge = jnp.maximum(scaled, float(k))
                absorbed = absorbed + a_bend[k] * hinge
                emitted = emitted + e_bend[k] * hinge
            absorbed = absorbed * occ[c]
            after = through[c] * jnp.exp2(absorbed)
            new_light.append(light[c] + (through[c] - after) * emitted)
            new_depth.append(depth[c] + absorbed)
            new_through.append(after)
        return new_through, new_depth, new_light

    cws = [col_weights(c) for c in range(tiles)]

    def tile_of(c):
        return slice(c * LANES, (c + 1) * LANES)

    def plane(z, t, rw):
        def own(c):
            return dens[z, t * SUB : (t + 1) * SUB, tile_of(c)]

        def following(c):
            if t + 1 < row_tiles:
                nxt = dens[z, (t + 1) * SUB : (t + 1) * SUB + 1, tile_of(c)]
            else:
                nxt = row_halo[z, 0:1, tile_of(c)]
            return jnp.broadcast_to(nxt, (SUB, LANES))

        return resampled(own, following, rw, cws)

    def last_plane(t, rw):
        def own(c):
            return below[t * SUB : (t + 1) * SUB, tile_of(c)]

        def following(c):
            if t + 1 < row_tiles:
                nxt = below[(t + 1) * SUB : (t + 1) * SUB + 1, tile_of(c)]
            else:
                nxt = corner[0:1, tile_of(c)]
            return jnp.broadcast_to(nxt, (SUB, LANES))

        return resampled(own, following, rw, cws)

    def march(t, first, last, carry):
        rw = row_weights(t)
        if carry is None:
            ones = [jnp.ones((SUB, LANES), jnp.float32)] * tiles
            zeros = [jnp.zeros((SUB, LANES), jnp.float32)] * tiles
            carry = (plane(0, t, rw), (ones, zeros, zeros))

        def step(z, carry):
            prev, state = carry
            now = plane(z, t, rw)
            return now, shade(prev, now, state)

        return lax.fori_loop(first, last, step, carry)

    def finish(t, carry):
        prev, state = carry
        _, depth, light = shade(prev, last_plane(t, row_weights(t)), state)
        for c in range(tiles):
            j, at = (c * LANES) // width, (c * LANES) % width
            parts[t, j, 0, :, at : at + LANES] = depth[c]
            parts[t, j, 1, :, at : at + LANES] = light[c]

    load.wait()
    for z in range(slab):
        row_send[z] = dens[z, 0:1, :]
    corner_send[...] = dens[0, 0:1, :]
    half = slab // 2
    states = [None] * row_tiles
    states[0] = march(0, 1, half, None)

    pl.semaphore_wait(barrier, n_depth - 1 + 4)

    def halo(k, src, dst, dd, dr):
        return pltpu.make_async_remote_copy(
            src_ref=src,
            dst_ref=dst,
            send_sem=halo_send_sem.at[k],
            recv_sem=halo_recv_sem.at[k],
            device_id=shifted(dd, dr),
            device_id_type=MESH,
        )

    depth_copy = halo(0, dens.at[0], below, -1, 0)
    rows_copy = halo(1, row_send, row_halo, 0, -1)
    corner_copy = halo(2, corner_send, corner, -1, -1)
    sends = (
        (depth_copy, d > 0, d < n_depth - 1),
        (rows_copy, r > 0, r < n_rows - 1),
        (
            corner_copy,
            jnp.logical_and(d > 0, r > 0),
            jnp.logical_and(d < n_depth - 1, r < n_rows - 1),
        ),
    )
    for copy, sending, _ in sends:
        pl.when(sending)(copy.start)

    def other(i):
        return lax.rem(d + 1 + i, n_depth)

    def when_owner(index, body):
        if owners == n_depth:
            body()
        else:
            pl.when(index < owners)(body)

    def part_copy(t, owner, source):
        return pltpu.make_async_remote_copy(
            src_ref=parts.at[t, owner],
            dst_ref=gathered.at[t, source],
            send_sem=part_send_sem.at[t, owner],
            recv_sem=part_recv_sem.at[t, source],
            device_id=(owner, r),
            device_id_type=MESH,
        )

    def answer_copy(t, target, owner):
        return pltpu.make_async_remote_copy(
            src_ref=answers.at[t, target],
            dst_ref=results.at[t, owner],
            send_sem=ans_send_sem.at[t, target],
            recv_sem=ans_recv_sem.at[t, owner],
            device_id=(target, r),
            device_id_type=MESH,
        )

    def send_parts(t):
        def send(i):
            when_owner(other(i), lambda: part_copy(t, other(i), d).start())

        repeat(n_depth - 1, send)

    def compose(t):
        gathered[t, pl.ds(d, 1)] = parts[t, pl.ds(d, 1)]

        def arrived(i):
            part_copy(t, d, other(i)).wait_recv()

        repeat(n_depth - 1, arrived)

        def add(i, carry):
            total, radiance = carry
            front = jnp.exp2(total)
            answers[t, i, 0] = front
            return total + gathered[t, i, 0], radiance + front * gathered[t, i, 1]

        zero = jnp.zeros((SUB, width), jnp.float32)
        carry = (zero, zero)
        if n_depth <= 16:
            for i in range(n_depth):
                carry = add(i, carry)
        else:
            carry = lax.fori_loop(0, n_depth, add, carry)
        total, radiance = carry
        remaining = jnp.exp2(total)

        def fill(i):
            answers[t, i, 1] = radiance
            answers[t, i, 2] = remaining

        repeat(n_depth, fill)

        def reply(i):
            answer_copy(t, other(i), d).start()

        repeat(n_depth - 1, reply)
        results[t, pl.ds(d, 1)] = answers[t, pl.ds(d, 1)]

    states[0] = march(0, half, slab, states[0])
    pl.when(sends[1][2])(rows_copy.wait_recv)
    for t in range(row_tiles):
        last = t == row_tiles - 1
        if not last:
            states[t + 1] = march(t + 1, 1, half, None)
        if t == 0:
            pl.when(sends[0][2])(depth_copy.wait_recv)
            pl.when(sends[2][2])(corner_copy.wait_recv)
        finish(t, states[t])
        send_parts(t)
        if not last:
            states[t + 1] = march(t + 1, half, slab, states[t + 1])

    for t in range(row_tiles):
        when_owner(d, functools.partial(compose, t))

    for t in range(row_tiles):

        def collect(i):
            when_owner(other(i), lambda: answer_copy(t, d, other(i)).wait_recv())

        repeat(n_depth - 1, collect)

    for copy, sending, _ in sends:
        pl.when(sending)(copy.wait_send)

    for t in range(row_tiles):

        def sent(i):
            when_owner(other(i), lambda: part_copy(t, other(i), d).wait_send())
            when_owner(d, lambda: answer_copy(t, other(i), d).wait_send())

        repeat(n_depth - 1, sent)


def lay_out(results, front_ref, image_ref):
    row_tiles, owners, _, _, width = results.shape
    for t in range(row_tiles):
        for j in range(owners):
            tall, where = slice(t * SUB, (t + 1) * SUB), slice(j * width, (j + 1) * width)
            front_ref[0, tall, where] = results[t, j, 0]
            image_ref[0, tall, where] = results[t, j, 1]
            image_ref[1, tall, where] = results[t, j, 2]


def on_device(n_depth, n_rows, density, bin_of_level, absorb_bins, emit_bins, occupancy, col_offsets, row_offsets):
    slab, rows, cols = density.shape
    owners = 1
    while owners * 2 <= n_depth and cols % (owners * 2 * LANES) == 0:
        owners *= 2
    width = cols // owners
    row_tiles = rows // SUB
    smem = pl.BlockSpec(memory_space=pltpu.SMEM)
    vmem = pl.BlockSpec(memory_space=pltpu.VMEM)
    f32 = jnp.float32
    results = pl.pallas_call(
        functools.partial(kernel, n_depth, n_rows),
        out_shape=pltpu.VMEM((row_tiles, owners, 3, SUB, width), f32),
        in_specs=[pl.BlockSpec(memory_space=pl.ANY), smem, smem, smem, smem, vmem, smem],
        out_specs=vmem,
        scratch_shapes=[
            pltpu.VMEM((slab, rows, cols), f32),
            pltpu.VMEM((rows, cols), f32),
            pltpu.VMEM((slab, 1, cols), f32),
            pltpu.VMEM((slab, 1, cols), f32),
            pltpu.VMEM((1, cols), f32),
            pltpu.VMEM((1, cols), f32),
            pltpu.VMEM((row_tiles, owners, 2, SUB, width), f32),
            pltpu.VMEM((row_tiles, n_depth, 2, SUB, width), f32),
            pltpu.VMEM((row_tiles, n_depth, 3, SUB, width), f32),
            pltpu.SemaphoreType.DMA,
            pltpu.SemaphoreType.DMA((3,)),
            pltpu.SemaphoreType.DMA((3,)),
            pltpu.SemaphoreType.DMA((row_tiles, owners)),
            pltpu.SemaphoreType.DMA((row_tiles, n_depth)),
            pltpu.SemaphoreType.DMA((row_tiles, n_depth)),
            pltpu.SemaphoreType.DMA((row_tiles, owners)),
        ],
        compiler_params=pltpu.CompilerParams(collective_id=0, has_side_effects=True),
    )(
        density,
        bin_of_level,
        absorb_bins,
        emit_bins,
        occupancy,
        col_offsets.reshape(1, cols),
        row_offsets,
    )
    laid = results.transpose(2, 0, 3, 1, 4).reshape(3, rows, cols)
    return laid[:1], laid[1:]


def solution(mesh):
    placed = (P("depth", "rows", None), P(), P(), P(), P("depth", "rows", None), P(), P("rows"))
    return jax.shard_map(
        functools.partial(on_device, mesh.shape["depth"], mesh.shape["rows"]),
        mesh=mesh,
        in_specs=placed,
        out_specs=(P("depth", "rows", None), P(None, "rows", None)),
        check_vma=False,
    )
```

```python
import functools
import math

import jax
import jax.numpy as jnp
from jax import lax
from jax.experimental import pallas as pl
from jax.experimental.pallas import tpu as pltpu
from jax.sharding import PartitionSpec as P

LANES = 128
SUB = 8
MESH = pl.DeviceIdType.MESH


def repeat(count, body):
    if count <= 16:
        for i in range(count):
            body(i)
    else:
        lax.fori_loop(0, count, lambda i, c: (body(i), c)[1], 0)


def kernel(
    n_depth,
    n_rows,
    dens_hbm,
    bins_ref,
    absorb_ref,
    emit_ref,
    occ_ref,
    col_ref,
    row_ref,
    results,
    dens,
    below,
    row_send,
    row_halo,
    corner_send,
    corner,
    parts,
    gathered,
    answers,
    load_sem,
    halo_send_sem,
    halo_recv_sem,
    part_send_sem,
    part_recv_sem,
    ans_send_sem,
    ans_recv_sem,
):
    slab, rows, cols = dens.shape
    owners = parts.shape[1]
    width = cols // owners
    tiles = cols // LANES
    row_tiles = rows // SUB
    levels = bins_ref.shape[0]
    d = lax.axis_index("depth")
    r = lax.axis_index("rows")

    def shifted(dd, dr):
        return (lax.rem(d + dd + n_depth, n_depth), lax.rem(r + dr + n_rows, n_rows))

    load = pltpu.make_async_copy(dens_hbm, dens, load_sem)
    load.start()

    barrier = pltpu.get_barrier_semaphore()
    for dd, dr in ((0, -1), (0, 1), (-1, -1), (1, 1)):
        pl.semaphore_signal(barrier, inc=1, device_id=shifted(dd, dr), device_id_type=MESH)

    def greet(i):
        pl.semaphore_signal(
            barrier, inc=1, device_id=(lax.rem(d + 1 + i, n_depth), r), device_id_type=MESH
        )

    repeat(n_depth - 1, greet)

    @pl.when(d == n_depth - 1)
    def _():
        below[...] = jnp.zeros_like(below)

    @pl.when(r == n_rows - 1)
    def _():
        row_halo[...] = jnp.zeros_like(row_halo)

    @pl.when(jnp.logical_or(d == n_depth - 1, r == n_rows - 1))
    def _():
        corner[...] = jnp.zeros_like(corner)

    lane = lax.broadcasted_iota(jnp.int32, (SUB, LANES), 1)
    sub = lax.broadcasted_iota(jnp.int32, (SUB, LANES), 0)
    to_log2 = -math.log2(math.e)
    absorb = [absorb_ref[bins_ref[k]] * to_log2 for k in range(levels)]
    emit = [emit_ref[bins_ref[k]] for k in range(levels)]

    def hinges(values):
        steps = [values[k + 1] - values[k] for k in range(levels - 1)]
        bend = steps[:1] + [steps[k] - steps[k - 1] for k in range(1, levels - 1)]
        shift = values[0]
        for k in range(1, levels - 1):
            shift = shift - bend[k] * float(k)
        return shift, bend

    a_shift, a_bend = hinges(absorb)
    e_shift, e_bend = hinges(emit)
    occ = [occ_ref[0, 0, (c * LANES) // (cols // occ_ref.shape[2])].astype(jnp.float32) for c in range(tiles)]

    def row_weights(t):
        frac = jnp.zeros((SUB, LANES), jnp.float32)
        for y in range(SUB):
            frac = jnp.where(sub == y, row_ref[t * SUB + y].astype(jnp.float32), frac)
        frac = frac / 8.0
        gain = 0.5 * float(levels - 1)
        return gain * (1.0 - frac), gain * frac

    def col_weights(c):
        frac = col_ref[0:1, c * LANES : (c + 1) * LANES].astype(jnp.float32) / 8.0
        frac = jnp.broadcast_to(frac, (SUB, LANES))
        keep = 1.0 - frac
        if c == tiles - 1:
            frac = jnp.where(lane == LANES - 1, 0.0, frac)
        return keep, frac

    def resampled(own, following, rw, cws):
        mixed = []
        for c in range(tiles):
            block = own(c)
            up = jnp.where(sub == SUB - 1, following(c), pltpu.roll(block, SUB - 1, 0))
            mixed.append(rw[0] * block + rw[1] * up)
        turned = [pltpu.roll(m, LANES - 1, 1) for m in mixed]
        out = []
        for c in range(tiles):
            right = jnp.where(lane == LANES - 1, turned[(c + 1) % tiles], turned[c])
            out.append(cws[c][0] * mixed[c] + cws[c][1] * right)
        return out

    def shade(prev, now, state):
        through, depth, light = state
        new_through, new_depth, new_light = [], [], []
        for c in range(tiles):
            scaled = prev[c] + now[c]
            absorbed = a_shift + a_bend[0] * scaled
            emitted = e_shift + e_bend[0] * scaled
            for k in range(1, levels - 1):
                hinge = jnp.maximum(scaled, float(k))
                absorbed = absorbed + a_bend[k] * hinge
                emitted = emitted + e_bend[k] * hinge
            absorbed = absorbed * occ[c]
            after = through[c] * jnp.exp2(absorbed)
            new_light.append(light[c] + (through[c] - after) * emitted)
            new_depth.append(depth[c] + absorbed)
            new_through.append(after)
        return new_through, new_depth, new_light

    cws = [col_weights(c) for c in range(tiles)]

    def tile_of(c):
        return slice(c * LANES, (c + 1) * LANES)

    def plane(z, t, rw):
        def own(c):
            return dens[z, t * SUB : (t + 1) * SUB, tile_of(c)]

        def following(c):
            if t + 1 < row_tiles:
                nxt = dens[z, (t + 1) * SUB : (t + 1) * SUB + 1, tile_of(c)]
            else:
                nxt = row_halo[z, 0:1, tile_of(c)]
            return jnp.broadcast_to(nxt, (SUB, LANES))

        return resampled(own, following, rw, cws)

    def last_plane(t, rw):
        def own(c):
            return below[t * SUB : (t + 1) * SUB, tile_of(c)]

        def following(c):
            if t + 1 < row_tiles:
                nxt = below[(t + 1) * SUB : (t + 1) * SUB + 1, tile_of(c)]
            else:
                nxt = corner[0:1, tile_of(c)]
            return jnp.broadcast_to(nxt, (SUB, LANES))

        return resampled(own, following, rw, cws)

    def march(t, first, last, carry):
        rw = row_weights(t)
        if carry is None:
            ones = [jnp.ones((SUB, LANES), jnp.float32)] * tiles
            zeros = [jnp.zeros((SUB, LANES), jnp.float32)] * tiles
            carry = (plane(0, t, rw), (ones, zeros, zeros))

        def step(z, carry):
            prev, state = carry
            now = plane(z, t, rw)
            return now, shade(prev, now, state)

        return lax.fori_loop(first, last, step, carry)

    def finish(t, carry):
        prev, state = carry
        _, depth, light = shade(prev, last_plane(t, row_weights(t)), state)
        for c in range(tiles):
            j, at = (c * LANES) // width, (c * LANES) % width
            parts[t, j, 0, :, at : at + LANES] = depth[c]
            parts[t, j, 1, :, at : at + LANES] = light[c]

    load.wait()
    for z in range(slab):
        row_send[z] = dens[z, 0:1, :]
    corner_send[...] = dens[0, 0:1, :]
    half = slab // 2
    states = [None] * row_tiles
    states[0] = march(0, 1, half, None)

    pl.semaphore_wait(barrier, n_depth - 1 + 4)

    def halo(k, src, dst, dd, dr):
        return pltpu.make_async_remote_copy(
            src_ref=src,
            dst_ref=dst,
            send_sem=halo_send_sem.at[k],
            recv_sem=halo_recv_sem.at[k],
            device_id=shifted(dd, dr),
            device_id_type=MESH,
        )

    depth_copy = halo(0, dens.at[0], below, -1, 0)
    rows_copy = halo(1, row_send, row_halo, 0, -1)
    corner_copy = halo(2, corner_send, corner, -1, -1)
    sends = (
        (depth_copy, d > 0, d < n_depth - 1),
        (rows_copy, r > 0, r < n_rows - 1),
        (
            corner_copy,
            jnp.logical_and(d > 0, r > 0),
            jnp.logical_and(d < n_depth - 1, r < n_rows - 1),
        ),
    )
    for copy, sending, _ in sends:
        pl.when(sending)(copy.start)

    def other(i):
        return lax.rem(d + 1 + i, n_depth)

    def when_owner(index, body):
        if owners == n_depth:
            body()
        else:
            pl.when(index < owners)(body)

    def part_copy(t, owner, source):
        return pltpu.make_async_remote_copy(
            src_ref=parts.at[t, owner],
            dst_ref=gathered.at[t, source],
            send_sem=part_send_sem.at[t, owner],
            recv_sem=part_recv_sem.at[t, source],
            device_id=(owner, r),
            device_id_type=MESH,
        )

    def answer_copy(t, target, owner):
        return pltpu.make_async_remote_copy(
            src_ref=answers.at[t, target],
            dst_ref=results.at[t, owner],
            send_sem=ans_send_sem.at[t, target],
            recv_sem=ans_recv_sem.at[t, owner],
            device_id=(target, r),
            device_id_type=MESH,
        )

    def send_parts(t):
        def send(i):
            when_owner(other(i), lambda: part_copy(t, other(i), d).start())

        repeat(n_depth - 1, send)

    def compose(t):
        gathered[t, pl.ds(d, 1)] = parts[t, pl.ds(d, 1)]

        def arrived(i):
            part_copy(t, d, other(i)).wait_recv()

        repeat(n_depth - 1, arrived)

        def add(i, carry):
            total, radiance = carry
            front = jnp.exp2(total)
            answers[t, i, 0] = front
            return total + gathered[t, i, 0], radiance + front * gathered[t, i, 1]

        zero = jnp.zeros((SUB, width), jnp.float32)
        carry = (zero, zero)
        if n_depth <= 16:
            for i in range(n_depth):
                carry = add(i, carry)
        else:
            carry = lax.fori_loop(0, n_depth, add, carry)
        total, radiance = carry
        remaining = jnp.exp2(total)

        def fill(i):
            answers[t, i, 1] = radiance
            answers[t, i, 2] = remaining

        repeat(n_depth, fill)

        def reply(i):
            answer_copy(t, other(i), d).start()

        repeat(n_depth - 1, reply)
        results[t, pl.ds(d, 1)] = answers[t, pl.ds(d, 1)]

    states[0] = march(0, half, slab, states[0])
    pl.when(sends[1][2])(rows_copy.wait_recv)
    for t in range(row_tiles):
        last = t == row_tiles - 1
        if not last:
            states[t + 1] = march(t + 1, 1, slab // 4, None)
        if t == 0:
            pl.when(sends[0][2])(depth_copy.wait_recv)
            pl.when(sends[2][2])(corner_copy.wait_recv)
        finish(t, states[t])
        send_parts(t)
        if not last:
            states[t + 1] = march(t + 1, slab // 4, slab, states[t + 1])

    for t in range(row_tiles):
        when_owner(d, functools.partial(compose, t))

    for t in range(row_tiles):

        def collect(i):
            when_owner(other(i), lambda: answer_copy(t, d, other(i)).wait_recv())

        repeat(n_depth - 1, collect)

    for copy, sending, _ in sends:
        pl.when(sending)(copy.wait_send)

    for t in range(row_tiles):

        def sent(i):
            when_owner(other(i), lambda: part_copy(t, other(i), d).wait_send())
            when_owner(d, lambda: answer_copy(t, other(i), d).wait_send())

        repeat(n_depth - 1, sent)


def lay_out(results, front_ref, image_ref):
    row_tiles, owners, _, _, width = results.shape
    for t in range(row_tiles):
        for j in range(owners):
            tall, where = slice(t * SUB, (t + 1) * SUB), slice(j * width, (j + 1) * width)
            front_ref[0, tall, where] = results[t, j, 0]
            image_ref[0, tall, where] = results[t, j, 1]
            image_ref[1, tall, where] = results[t, j, 2]


def on_device(n_depth, n_rows, density, bin_of_level, absorb_bins, emit_bins, occupancy, col_offsets, row_offsets):
    slab, rows, cols = density.shape
    owners = 1
    while owners * 2 <= n_depth and cols % (owners * 2 * LANES) == 0:
        owners *= 2
    width = cols // owners
    row_tiles = rows // SUB
    smem = pl.BlockSpec(memory_space=pltpu.SMEM)
    vmem = pl.BlockSpec(memory_space=pltpu.VMEM)
    f32 = jnp.float32
    results = pl.pallas_call(
        functools.partial(kernel, n_depth, n_rows),
        out_shape=pltpu.VMEM((row_tiles, owners, 3, SUB, width), f32),
        in_specs=[pl.BlockSpec(memory_space=pl.ANY), smem, smem, smem, smem, vmem, smem],
        out_specs=vmem,
        scratch_shapes=[
            pltpu.VMEM((slab, rows, cols), f32),
            pltpu.VMEM((rows, cols), f32),
            pltpu.VMEM((slab, 1, cols), f32),
            pltpu.VMEM((slab, 1, cols), f32),
            pltpu.VMEM((1, cols), f32),
            pltpu.VMEM((1, cols), f32),
            pltpu.VMEM((row_tiles, owners, 2, SUB, width), f32),
            pltpu.VMEM((row_tiles, n_depth, 2, SUB, width), f32),
            pltpu.VMEM((row_tiles, n_depth, 3, SUB, width), f32),
            pltpu.SemaphoreType.DMA,
            pltpu.SemaphoreType.DMA((3,)),
            pltpu.SemaphoreType.DMA((3,)),
            pltpu.SemaphoreType.DMA((row_tiles, owners)),
            pltpu.SemaphoreType.DMA((row_tiles, n_depth)),
            pltpu.SemaphoreType.DMA((row_tiles, n_depth)),
            pltpu.SemaphoreType.DMA((row_tiles, owners)),
        ],
        compiler_params=pltpu.CompilerParams(collective_id=0, has_side_effects=True),
    )(
        density,
        bin_of_level,
        absorb_bins,
        emit_bins,
        occupancy,
        col_offsets.reshape(1, cols),
        row_offsets,
    )
    laid = results.transpose(2, 0, 3, 1, 4).reshape(3, rows, cols)
    return laid[:1], laid[1:]


def solution(mesh):
    placed = (P("depth", "rows", None), P(), P(), P(), P("depth", "rows", None), P(), P("rows"))
    return jax.shard_map(
        functools.partial(on_device, mesh.shape["depth"], mesh.shape["rows"]),
        mesh=mesh,
        in_specs=placed,
        out_specs=(P("depth", "rows", None), P(None, "rows", None)),
        check_vma=False,
    )
```
